32 devices in a mesh: dev: 32 (over z, y, x, core).
Axes of the slice: x: 2, y: 2, z: 4, core: 2. Of those that a mesh axis runs over, the one named last changes fastest.
Arguments:
- state: float32 [128, 512, 128], P('dev'), may hold values from -6 to 6
- background: float32 [128, 512, 128], P('dev'), may hold values from -6 to 6
- back_precision: float32 [128], replicated, may hold values from 0.2 to 2
- conv_first: bfloat16 [3, 3, 128, 128], replicated, may hold values from -0.1875 to 0.1875
- bias_first: float32 [128], replicated, may hold values from -3 to 3
- conv_second: bfloat16 [3, 3, 128, 128], replicated, may hold values from -0.1875 to 0.1875
- sounding_tile: int32 [16384, 1], P('dev'), may hold values from 0 to 31; in each aligned block of 512 rows (0 to 511, 512 to 1023, ...) at most 32 rows name the same one
- sounding_cells: int32 [16384, 4], P('dev'), may hold values from 0 to 2047
- cell_weights: float32 [16384, 4], P('dev'), may hold values from 0.1 to 1
- observations: float32 [16384, 616], P('dev'), may hold values from -6 to 6
- live_counts: int32 [32], P('dev'), may hold values from 1 to 511, as said below
- layer_in: bfloat16 [128, 1024], replicated, may hold values from -0.5 to 0.5
- bias_in: float32 [1024], replicated, may hold values from -3 to 3
- layer_out: bfloat16 [1024, 616], replicated, may hold values from -0.1875 to 0.1875
- bias_out: float32 [616], replicated, may hold values from -3 to 3
- error_precision: float32 [616, 616], replicated, as said below
Outputs:
- gradient: float32 [128, 512, 128], P('dev')
The draws below stay inside these ranges and needn't reach their ends.
Inputs may be any that keep to these rules, and one draw needn't show every extreme that they name: `sounding_tile`: among the 512 soundings of one list, at most 32 lie in the same strip, and in some lists some strip holds exactly 32 of them. The live soundings of a list are its first live_counts; the counts of lists l and l + 16 sum to 512. `error_precision`: Symmetric.
All inputs are finite; a program needn't handle non-finite values.
Results may differ from the reference program's by a relative error of at most 0.008.
Values may be sent and summed in bfloat16 or wider, within the bound.
A program may use at most 64 MiB of HBM per device.

```python
import math
import jax
import jax.numpy as jnp
import numpy as np
from jax import lax

CH = 128
HID = 1024
NCHAN = 616
NCOLS = 512
MARGIN = 4
ROWS_DEV = 4
SND_DEV = 512
LISTS = 32
NROWS = 128
SOUNDINGS = 16384
CAP = 32
N_DEV = 32


def draw_live_counts(key, part):
    half_lists = LISTS // 2
    first_half = jax.random.randint(key, (half_lists,), 1, SND_DEV, dtype=jnp.int32)
    return jnp.concatenate([first_half, SND_DEV - first_half])


def draw_error_precision(key, part):
    key_off, key_diag = jax.random.split(jax.random.fold_in(key, 17))
    draws_raw = jax.random.normal(key_off, (NCHAN, NCHAN), jnp.float32)
    off_part = (draws_raw + draws_raw.T) * (0.35 / math.sqrt(NCHAN))
    diagonal = jax.random.uniform(key_diag, (NCHAN,), jnp.float32, 1.0, 3.0)
    return off_part + jnp.diag(diagonal)


def plant(drawn, own_key, low, largest):
    index_at = [jax.random.randint(jax.random.fold_in(own_key, axis), (), 0, length) for axis, length in enumerate(drawn.shape)]
    main_axis = drawn.shape.index(max(drawn.shape))
    beside = index_at[:main_axis] + [(index_at[main_axis] + 1) % drawn.shape[main_axis]] + index_at[main_axis + 1:]
    return drawn.at[tuple(index_at)].set(low).at[tuple(beside)].set(largest)


def level_of(rng, shape, cuts, low, high):
    def one(axis_at, blocks):
        steps = jax.random.uniform(jax.random.fold_in(jax.random.fold_in(rng, 6), axis_at), (blocks,), jnp.float32, low / len(cuts), high / len(cuts))
        return jnp.repeat(jnp.exp(steps), shape[axis_at] // blocks).reshape((-1,) + (1,) * (len(shape) - axis_at - 1))

    factor_of = one(*cuts[0])
    for cut in cuts[1:]:
        factor_of = factor_of * one(*cut)
    return factor_of


def routed_block(key, own, number, rows, count, top, most, slope):
    order = jax.random.permutation(key, count)
    crowded, ordinary = portions_of(count, rows * top, most, slope, True), portions_of(count, rows * top, most, slope, False)
    places = jnp.arange(count)

    def named(sizes, rotation):
        used = int((sizes > 0).sum())
        fixed = max(1, used // 4)
        moved = fixed + (places - fixed + rotation * (used - fixed)) % max(1, count - fixed)
        return jnp.zeros((count,), jnp.int32).at[order[jnp.where(places < fixed, places, moved)]].set(jnp.asarray(sizes, jnp.int32))

    sizes = jnp.where(number % 4 == 0, named(crowded, number // 4), named(ordinary, number - number // 4 - 1))
    mixed = jax.random.permutation(jax.random.fold_in(own, 3), count)
    donor, receiver = mixed[0:count // 2 * 2:2], mixed[1:count // 2 * 2:2]
    margin = jnp.minimum(sizes[donor] - 1, most - sizes[receiver]) // 2
    margin = jnp.where((donor == order[0]) | (receiver == order[0]) | (sizes[receiver] == 0), 0, jnp.maximum(margin, 0))
    moved = jax.random.randint(jax.random.fold_in(own, 4), (count // 2,), 0, 1 << 20) % (margin + 1)
    sizes = sizes.at[donor].add(-moved).at[receiver].add(moved)
    items = jnp.searchsorted(jnp.cumsum(sizes), jnp.arange(rows * top), side="right").astype(jnp.int32)
    listing = items.reshape(top, rows).T
    listing = listing[jax.random.permutation(jax.random.fold_in(own, 1), rows)]
    rotation = jax.random.randint(jax.random.fold_in(own, 2), (rows, 1), 0, top)
    return jnp.take_along_axis(listing, (jnp.arange(top)[None, :] + rotation) % top, axis=1)


def portions_of(amount, total, reach, lean, full):
    portions = [(1 << 20) // math.isqrt(standing ** lean) + 1 for standing in range(1, amount + 1)]
    largest = reach if full else min(reach, max(-(-total // amount), total * portions[0] // sum(portions)))
    least = 1 if total - largest >= amount - 1 else 0
    holding, spare = [largest] + [least] * (amount - 1), total - largest - least * (amount - 1)
    while spare > 0:
        movable = [i for i in range(1, amount) if holding[i] < largest] or [i for i in range(1, amount) if holding[i] < reach]
        pool, left = sum([portions[i] for i in movable]), spare
        for i in movable:
            more = min(reach - holding[i], max(1, left * portions[i] // pool), spare)
            holding[i] = holding[i] + more
            spare = spare - more
    return np.array(holding)


def bell_draw(rng, dims, deviation, bound, pieces=(), held_as=jnp.bfloat16):
    array = jax.random.normal(rng, dims, jnp.float32) * deviation
    if len(pieces) > 0:
        array = level_of(rng, dims, pieces, -0.22, 0.18) * array
    return jnp.clip(array, min=-bound, max=bound).astype(held_as)


def setup_inputs(seed: int = 0) -> dict:
    key_list = jax.random.split(jax.random.key(seed), 17)
    state = bell_draw(key_list[0], (NROWS, NCOLS, CH), 1.0, 6.0, ((0, 32),), jnp.float32)
    background = bell_draw(key_list[1], (NROWS, NCOLS, CH), 1.0, 6.0, ((0, 32),), jnp.float32)
    back_precision = jnp.clip(jnp.exp(jax.random.uniform(key_list[2], (CH,), jnp.float32, math.log(0.2), math.log(2.0))), 0.2, 2.0)
    conv_first = bell_draw(key_list[3], (3, 3, CH, CH), (9 * CH) ** -0.5, 0.1875)
    bias_first = bell_draw(key_list[4], (CH,), 0.5, 3.0, (), jnp.float32)
    conv_second = bell_draw(key_list[5], (3, 3, CH, CH), (9 * CH) ** -0.5, 0.1875)
    sounding_tile_keys = jax.random.split(jax.random.fold_in(key_list[6], 1), SOUNDINGS // SND_DEV)
    sounding_tile_turns = jax.random.permutation(jax.random.fold_in(key_list[6], 3), SOUNDINGS // SND_DEV)
    sounding_tile = jax.vmap(lambda own, number: routed_block(jax.random.fold_in(key_list[6], 2), own, number, SND_DEV, LISTS, 1, CAP, 2))(sounding_tile_keys, sounding_tile_turns).reshape((SOUNDINGS, 1))
    sounding_cells = plant(jax.random.randint(key_list[7], (SOUNDINGS, MARGIN), 0, ROWS_DEV * NCOLS), jax.random.fold_in(key_list[7], 1), 0, (ROWS_DEV * NCOLS) - 1).astype(jnp.int32)
    cell_weights = jnp.clip(jnp.exp(math.log(1.0) - 2.3025851 * jax.random.uniform(key_list[8], (SOUNDINGS, MARGIN), jnp.float32) ** level_of(key_list[8], (SOUNDINGS, MARGIN), ((0, 32),), -0.2, 0.2)), 0.1, 1.0)
    observations = bell_draw(key_list[9], (SOUNDINGS, NCHAN), 1.0, 6.0, ((0, 32),), jnp.float32)
    live_counts = draw_live_counts(jax.random.fold_in(key_list[16], 71), 0)
    layer_in = bell_draw(key_list[11], (CH, HID), CH ** -0.5, 0.5)
    bias_in = bell_draw(key_list[12], (HID,), 0.5, 3.0, (), jnp.float32)
    layer_out = bell_draw(key_list[13], (HID, NCHAN), HID ** -0.5, 0.1875)
    bias_out = bell_draw(key_list[14], (NCHAN,), 0.5, 3.0, (), jnp.float32)
    error_precision = draw_error_precision(jax.random.fold_in(key_list[16], 71), 0)
    return dict(state=state, background=background, back_precision=back_precision, conv_first=conv_first, bias_first=bias_first, conv_second=conv_second, sounding_tile=sounding_tile, sounding_cells=sounding_cells, cell_weights=cell_weights, observations=observations, live_counts=live_counts, layer_in=layer_in, bias_in=bias_in, layer_out=layer_out, bias_out=bias_out, error_precision=error_precision)


def conv_rows(padded, kernel):
    tile_rows = padded.shape[0] - 2
    channels = padded.shape[2]
    total = jnp.zeros((tile_rows * padded.shape[1], kernel.shape[3]), jnp.float32)
    for row_off in range(3):
        row_band = padded[row_off:row_off + tile_rows]
        for col_off in range(3):
            shifted = jnp.roll(row_band, 1 - col_off, axis=1)
            total = total + jnp.dot(shifted.reshape(-1, channels), kernel[row_off, col_off], preferred_element_type=jnp.float32)
    return total.reshape(tile_rows, padded.shape[1], kernel.shape[3])


def pad_rows(field_in):
    return jnp.pad(field_in, ((1, 1), (0, 0), (0, 0)))


def flipped(kernel):
    return kernel[::-1, ::-1].transpose(0, 1, 3, 2)


def reference(state, background, back_precision, conv_first, bias_first, conv_second, sounding_tile, sounding_cells, cell_weights, observations, live_counts, layer_in, bias_in, layer_out, bias_out, error_precision):
    state_bf = state.astype(jnp.bfloat16)
    hidden = jnp.tanh(conv_rows(pad_rows(state_bf), conv_first) + bias_first).astype(jnp.bfloat16)
    observed = (state + conv_rows(pad_rows(hidden), conv_second)).astype(jnp.bfloat16)
    observed_flat = observed.reshape(-1, CH)
    flat_index = (sounding_tile * (ROWS_DEV * NCOLS) + sounding_cells).astype(jnp.int32)
    positions = jnp.arange(SOUNDINGS, dtype=jnp.int32)
    live_mask = ((positions % SND_DEV) < jnp.repeat(live_counts, SND_DEV)).astype(jnp.float32)

    def one_block(bundle):
        indices, weights, measured, alive = bundle
        picked = observed_flat[indices].astype(jnp.float32)
        interpolated = jnp.sum(picked * weights[:, :, None], axis=1).astype(jnp.bfloat16)
        pre_act = jnp.dot(interpolated, layer_in, preferred_element_type=jnp.float32) + bias_in
        activated = jnp.tanh(pre_act).astype(jnp.bfloat16)
        radiance = jnp.dot(activated, layer_out, preferred_element_type=jnp.float32) + bias_out
        innovation = (radiance - measured) * alive[:, None]
        weighted = jnp.dot(innovation, error_precision, precision=lax.Precision.HIGHEST)
        back_act = jnp.dot(weighted.astype(jnp.bfloat16), layer_out.T, preferred_element_type=jnp.float32)
        act_wide = activated.astype(jnp.float32)
        pre_grad = (back_act * (1.0 - act_wide * act_wide)).astype(jnp.bfloat16)
        return jnp.dot(pre_grad, layer_in.T, preferred_element_type=jnp.float32)

    sounding_grad = lax.map(one_block, (
        flat_index.reshape(N_DEV, SND_DEV, MARGIN),
        cell_weights.reshape(N_DEV, SND_DEV, MARGIN),
        observations.reshape(N_DEV, SND_DEV, NCHAN),
        live_mask.reshape(N_DEV, SND_DEV))).reshape(SOUNDINGS, CH)
    ref_terms = cell_weights[:, :, None] * sounding_grad[:, None, :]
    obs_grad = jnp.zeros((NROWS * NCOLS, CH), jnp.float32).at[flat_index.reshape(-1)].add(ref_terms.reshape(-1, CH))
    obs_grad = obs_grad.reshape(state.shape)
    hid_grad = conv_rows(pad_rows(obs_grad.astype(jnp.bfloat16)), flipped(conv_second))
    hidden_wide = hidden.astype(jnp.float32)
    act_grad = (hid_grad * (1.0 - hidden_wide * hidden_wide)).astype(jnp.bfloat16)
    model_grad = conv_rows(pad_rows(act_grad), flipped(conv_first))
    return obs_grad + model_grad + back_precision * (state - background)
```

```python
import functools

import jax
import jax.numpy as jnp
from jax import lax
from jax.experimental import pallas as pl
from jax.experimental.pallas import tpu as pltpu
from jax.sharding import PartitionSpec as P

F32 = jnp.float32
BF16 = jnp.bfloat16
MESH = pl.DeviceIdType.MESH
LANES = 128


def dot(a, b):
    return jnp.dot(a, b, preferred_element_type=F32)


def dot_nt(a, b):
    return lax.dot_general(a, b, (((1,), (1,)), ((), ())), preferred_element_type=F32)


def kernel(
    n,
    live_ref,
    state_hbm,
    background_hbm,
    back_precision_hbm,
    conv_first_hbm,
    bias_first_hbm,
    conv_second_hbm,
    tile_hbm,
    cells_hbm,
    weights_hbm,
    observations_hbm,
    layer_in_hbm,
    bias_in_hbm,
    layer_out_hbm,
    bias_out_hbm,
    precision_hbm,
    out_ref,
    state_ref,
    background_ref,
    back_precision_ref,
    conv_first_ref,
    bias_first_ref,
    conv_second_ref,
    tile_ref,
    cells_ref,
    weights_ref,
    observations_ref,
    layer_in_ref,
    bias_in_ref,
    layer_out_ref,
    bias_out_ref,
    precision_ref,
    pair_first_ref,
    pair_second_ref,
    adj_first_ref,
    adj_second_ref,
    offset_ref,
    product_ref,
    field_ref,
    halo_ref,
    taps_ref,
    hidden_ref,
    hidden_taps_ref,
    partial_ref,
    edge_ref,
    observed_t_ref,
    values_ref,
    place_ref,
    place_t_ref,
    share_t_ref,
    grad_ref,
    req_src,
    req_dst,
    ret_src,
    ret_dst,
    out_src,
    out_dst,
    load_sem,
    halo_send,
    halo_recv,
    req_send,
    req_recv,
    ret_send,
    ret_recv,
    out_send,
    out_recv,
):
    me = lax.axis_index("dev")
    rows, cols, ch = state_ref.shape
    slots, listed = place_t_ref.shape
    cap = slots // n
    per = LANES // cap
    groups = slots // LANES
    half = n // 2
    span_half = slots // 2
    wide = 3 * ch
    margin = cells_ref.shape[0]
    my_half = lax.div(me, half)

    loads = [
        pltpu.make_async_copy(src, dst, load_sem.at[i])
        for i, (src, dst) in enumerate(
            (
                (tile_hbm, tile_ref),
                (cells_hbm, cells_ref),
                (weights_hbm, weights_ref),
                (state_hbm, state_ref),
                (conv_first_hbm, conv_first_ref),
                (bias_first_hbm, bias_first_ref),
                (precision_hbm, precision_ref),
                (layer_out_hbm, layer_out_ref),
                (conv_second_hbm, conv_second_ref),
                (observations_hbm, observations_ref),
                (bias_out_hbm, bias_out_ref),
                (background_hbm, background_ref),
                (back_precision_hbm, back_precision_ref),
                (layer_in_hbm, layer_in_ref),
                (bias_in_hbm, bias_in_ref),
            )
        )
    ]
    for load in loads:
        load.start()

    barrier = pltpu.get_barrier_semaphore()

    def greet(k, carry):
        pl.semaphore_signal(
            barrier, inc=1, device_id=(lax.rem(me + k, n),), device_id_type=MESH
        )
        return carry

    lax.fori_loop(1, n, greet, 0)

    def post(src, dst, send, recv, target):
        k = lax.rem(target + n - me, n)
        pltpu.make_async_remote_copy(
            src_ref=src.at[target],
            dst_ref=dst.at[me],
            send_sem=send.at[k],
            recv_sem=recv.at[k],
            device_id=(target,),
            device_id_type=MESH,
        ).start()

    def exchange_far(*refs):
        def start(j, carry):
            post(*refs, (1 - my_half) * half + lax.rem(me + j, half))
            return carry

        lax.fori_loop(0, half, start, 0)

    def exchange_near(*refs):
        def start(j, carry):
            post(*refs, my_half * half + lax.rem(me + j, half))
            return carry

        lax.fori_loop(1, half, start, 0)

    def settle(src, dst, send, recv):
        def wait(k, carry):
            copy = pltpu.make_async_remote_copy(
                src_ref=src.at[lax.rem(me + k, n)],
                dst_ref=dst.at[lax.rem(me + n - k, n)],
                send_sem=send.at[k],
                recv_sem=recv.at[k],
                device_id=(lax.rem(me + k, n),),
                device_id_type=MESH,
            )
            copy.wait_recv()
            copy.wait_send()
            return carry

        lax.fori_loop(1, n, wait, 0)

    def rim(phase, side, depth):
        row = (rows - 1 - depth) if side == 0 else depth
        return pltpu.make_async_remote_copy(
            src_ref=field_ref.at[phase, row],
            dst_ref=halo_ref.at[phase, side, depth],
            send_sem=halo_send.at[phase, side, depth],
            recv_sem=halo_recv.at[phase, side, depth],
            device_id=(lax.rem(me + 1, n) if side == 0 else lax.rem(me + n - 1, n),),
            device_id_type=MESH,
        )

    sends = (me < n - 1, me > 0)
    gets = (me > 0, me < n - 1)

    def rim_start(phase, depth):
        for side in range(2):

            @pl.when(sends[side])
            def _():
                rim(phase, side, depth).start()

    def rim_sent(phase, depth):
        for side in range(2):

            @pl.when(sends[side])
            def _():
                rim(phase, side, depth).wait_send()

    def put_taps(taps, slot, value):
        base = slot * wide
        taps[:, pl.ds(base, ch)] = pltpu.roll(value, 1, 0).astype(BF16)
        taps[:, pl.ds(base + ch, ch)] = value.astype(BF16)
        taps[:, pl.ds(base + 2 * ch, ch)] = pltpu.roll(value, cols - 1, 0).astype(BF16)

    def rim_take(phase, depth):
        for side in range(2):
            slot = (1 - depth) if side == 0 else rows + 2 + depth

            @pl.when(gets[side])
            def _():
                rim(phase, side, depth).wait_recv()
                put_taps(taps_ref, slot, halo_ref[phase, side, depth].astype(F32))

            @pl.when(jnp.logical_not(gets[side]))
            def _():
                taps_ref[:, pl.ds(slot * wide, wide)] = jnp.zeros((cols, wide), BF16)

    def make_pair(pair_ref, tap):
        zero = jnp.zeros((wide, ch), BF16)
        for a in range(4):
            for o in range(2):
                if 0 <= a - o < 3:
                    for b in range(3):
                        pair_ref[pl.ds(a * wide + b * ch, ch), pl.ds(o * ch, ch)] = tap(a - o, b)
                else:
                    pair_ref[pl.ds(a * wide, wide), pl.ds(o * ch, ch)] = zero

    def plain_of(ref):
        return lambda a, b: ref[a, pl.ds(b * ch, ch)]

    def adjoint_of(ref):
        return lambda a, b: ref[2 - a, pl.ds((2 - b) * ch, ch)].astype(F32).T.astype(BF16)

    def pair_all(taps, slot, pair):
        return dot(taps[:, pl.ds(slot * wide, 4 * wide)], pair[...])

    def pair_lower(taps, slot, pair):
        return dot(taps[:, pl.ds((slot + 1) * wide, 3 * wide)], pair[pl.ds(wide, 3 * wide)])

    def pair_upper(taps, slot, pair):
        return dot(taps[:, pl.ds(slot * wide, 3 * wide)], pair[pl.ds(0, 3 * wide)])

    def first_tap(taps, slot, pair):
        return dot(taps[:, pl.ds(slot * wide, wide)], pair[pl.ds(0, wide), pl.ds(0, ch)])

    def last_tap(taps, slot, pair):
        return dot(taps[:, pl.ds((slot + 2) * wide, wide)], pair[pl.ds(3 * wide, wide), pl.ds(ch, ch)])

    def outer_inside(pair, put):
        for slot in range(2, rows, 2):
            both = pair_all(taps_ref, slot, pair)
            put(slot, both[:, :ch])
            put(slot + 1, both[:, ch:])

    def outer_near(pair, put):
        both = pair_lower(taps_ref, 0, pair)
        partial_ref[0] = both[:, :ch]
        put(1, both[:, ch:])
        both = pair_upper(taps_ref, rows, pair)
        put(rows, both[:, :ch])
        partial_ref[1] = both[:, ch:]

    def outer_far(pair, put):
        put(0, (partial_ref[0] + first_tap(taps_ref, 0, pair)) * gets[0].astype(F32))
        put(rows + 1, (partial_ref[1] + last_tap(taps_ref, rows + 1, pair)) * gets[1].astype(F32))

    def inner_near(pair, put, put_edge):
        both = pair_lower(hidden_taps_ref, 0, pair)
        put_edge(0, both[:, :ch])
        put(1, both[:, ch:])
        for slot in range(2, rows - 2, 2):
            both = pair_all(hidden_taps_ref, slot, pair)
            put(slot, both[:, :ch])
            put(slot + 1, both[:, ch:])
        both = pair_upper(hidden_taps_ref, rows - 2, pair)
        put(rows - 2, both[:, :ch])
        put_edge(1, both[:, ch:])

    for load in loads[0:3]:
        load.wait()
    tile_row = tile_ref[...].astype(F32)
    tile_col = jnp.broadcast_to(tile_row, (LANES, listed)).T[:, 0:1]
    same = tile_col == tile_row
    from_col = lax.broadcasted_iota(jnp.int32, (listed, listed), 0)
    from_row = lax.broadcasted_iota(jnp.int32, (listed, listed), 1)
    rank_row = jnp.sum(jnp.where(same & (from_col < from_row), 1.0, 0.0), axis=0, keepdims=True)
    slot_row = (tile_row * cap + rank_row).astype(jnp.int32)
    for g in range(groups):
        rowid = lax.broadcasted_iota(jnp.int32, (LANES, listed), 0) + g * LANES
        place_t_ref[pl.ds(g * LANES, LANES)] = jnp.where(rowid == slot_row, 1.0, 0.0).astype(BF16)

    values_ref[0:margin] = cells_ref[...].astype(F32)
    values_ref[margin : 2 * margin] = weights_ref[...]
    values = values_ref[...]
    part_1 = values.astype(BF16).astype(F32)
    part_2 = (values - part_1).astype(BF16).astype(F32)
    part_3 = values - part_1 - part_2
    parts = jnp.concatenate([part_1, part_2, part_3, jnp.zeros_like(values)], axis=0).astype(BF16)
    own_lanes = lax.broadcasted_iota(jnp.int32, (8, LANES), 1) // cap == lax.rem(me, per)
    for g in range(groups):
        spread = dot_nt(parts, place_t_ref[pl.ds(g * LANES, LANES)])
        spread = spread[0:8] + spread[8:16] + spread[16:24]
        for i in range(per):
            turned = pltpu.roll(spread, lax.rem(lax.rem(me, per) + per - i, per) * cap, 1)
            req_src[g * per + i] = jnp.where(own_lanes, turned, 0.0)
    req_dst[me] = req_src[me]

    loads[3].wait()
    for r in range(rows):
        value = state_ref[r].astype(BF16)
        field_ref[0, r] = value
        put_taps(taps_ref, r + 2, value.astype(F32))

    def put_hidden(slot, value):
        inside = {0: gets[0], rows + 1: gets[1]}.get(slot)
        value = jnp.tanh(value + bias_first_ref[...]).astype(BF16).astype(F32)
        if inside is not None:
            value = value * inside.astype(F32)
        hidden_ref[slot] = value
        put_taps(hidden_taps_ref, slot, value)

    loads[4].wait()
    loads[5].wait()
    make_pair(pair_first_ref, plain_of(conv_first_ref))
    outer_inside(pair_first_ref, put_hidden)

    pl.semaphore_wait(barrier, n - 1)
    rim_start(0, 0)
    req = (req_src, req_dst, req_send, req_recv)
    exchange_far(*req)
    exchange_near(*req)
    rim_start(0, 1)

    loads[6].wait()
    loads[7].wait()
    chan = precision_ref.shape[0]
    step = 2 * LANES
    for s in range(0, chan, step):
        size = min(step, chan - s)
        wanted_rows = precision_ref[pl.ds(s, size)]
        high = wanted_rows.astype(BF16)
        low = (wanted_rows - high.astype(F32)).astype(BF16)
        product_ref[pl.ds(s, size)] = (
            dot(high, layer_out_ref[...]) + dot(low, layer_out_ref[...])
        ).astype(BF16)
    loads[8].wait()
    make_pair(pair_second_ref, plain_of(conv_second_ref))

    settle(*req)
    wanted = []
    for g in range(groups):
        total = req_dst[g * per]
        for i in range(1, per):
            total = total + req_dst[g * per + i]
        wanted.append(total)

    def build_shares(c, carry):
        base = pl.multiple_of(c * LANES, LANES)
        cell = lax.broadcasted_iota(jnp.int32, (LANES, LANES), 0).astype(F32)
        for g in range(groups):
            local = wanted[g] - base.astype(F32)
            total = jnp.zeros((LANES, LANES), F32)
            for k in range(margin):
                total = total + jnp.where(
                    cell == local[k : k + 1], wanted[g][margin + k : margin + k + 1], 0.0
                )
            share_t_ref[pl.ds(base, LANES), pl.ds(g * LANES, LANES)] = total.astype(BF16)
        return carry

    lax.fori_loop(0, rows * cols // LANES, build_shares, 0)

    rim_take(0, 0)
    outer_near(pair_first_ref, put_hidden)

    def put_observed(r, value):
        value = state_ref[r] + value
        observed_t_ref[:, pl.ds(r * cols, cols)] = value.T.astype(BF16)

    def hold_edge(side, value):
        edge_ref[side] = value

    inner_near(pair_second_ref, put_observed, hold_edge)
    rim_take(0, 1)

    def outer_far_forward():
        put_hidden(0, partial_ref[0] + first_tap(taps_ref, 0, pair_first_ref))
        put_hidden(rows + 1, partial_ref[1] + last_tap(taps_ref, rows + 1, pair_first_ref))

    outer_far_forward()
    put_observed(0, edge_ref[0] + first_tap(hidden_taps_ref, 0, pair_second_ref))
    put_observed(rows - 1, edge_ref[1] + last_tap(hidden_taps_ref, rows - 1, pair_second_ref))

    ret = (ret_src, ret_dst, ret_send, ret_recv)

    def blend(which):
        base = pl.multiple_of(which * span_half, span_half)
        blended = dot(observed_t_ref[...], share_t_ref[:, pl.ds(base, span_half)]).T
        ret_src[pl.ds(which * half, half)] = blended.reshape(half, cap, ch).astype(BF16)

    blend(1 - my_half)
    exchange_far(*ret)
    blend(my_half)
    exchange_near(*ret)
    ret_dst[me] = ret_src[me]

    rank_col = jnp.sum(jnp.where(same & (from_row < from_col), 1.0, 0.0), axis=1, keepdims=True)
    slot_col = (tile_col * cap + rank_col).astype(jnp.int32)
    for g in range(groups):
        colid = lax.broadcasted_iota(jnp.int32, (listed, LANES), 1) + g * LANES
        place_ref[:, pl.ds(g * LANES, LANES)] = jnp.where(colid == slot_col, 1.0, 0.0).astype(BF16)
    loads[9].wait()
    loads[10].wait()
    bias_out = bias_out_ref[...].reshape(1, -1)
    for s in range(0, listed, LANES):
        offset_ref[pl.ds(s, LANES)] = bias_out - observations_ref[:, pl.ds(s, LANES)].T
    make_pair(adj_second_ref, adjoint_of(conv_second_ref))
    make_pair(adj_first_ref, adjoint_of(conv_first_ref))
    loads[11].wait()
    loads[12].wait()
    for r in range(rows):
        out_ref[r] = back_precision_ref[...] * (state_ref[r] - background_ref[r])
    loads[13].wait()
    loads[14].wait()

    settle(*ret)
    returned = ret_dst[...].astype(F32).reshape(slots, ch).astype(BF16)
    live = live_ref[0]
    block = listed // 2
    for s in range(0, listed, block):
        span = pl.ds(s, block)
        interpolated = dot(place_ref[span], returned).astype(BF16)
        activated = jnp.tanh(dot(interpolated, layer_in_ref[...]) + bias_in_ref[...]).astype(BF16)
        innovation = dot_nt(activated, layer_out_ref[...]) + offset_ref[span]
        alive = lax.broadcasted_iota(jnp.int32, (block, 1), 0) + s < live
        innovation = jnp.where(alive, innovation, 0.0)
        back_act = dot(innovation.astype(BF16), product_ref[...])
        act_wide = activated.astype(F32)
        pre_grad = (back_act * (1.0 - act_wide * act_wide)).astype(BF16)
        grad_ref[span] = dot_nt(pre_grad, layer_in_ref[...]).astype(BF16)

    out = (out_src, out_dst, out_send, out_recv)

    def dispatch(which):
        base = pl.multiple_of(which * span_half, span_half)
        outgoing = dot(place_t_ref[pl.ds(base, span_half)], grad_ref[...])
        out_src[pl.ds(which * half, half)] = outgoing.reshape(half, cap, ch).astype(BF16)

    dispatch(1 - my_half)
    exchange_far(*out)
    dispatch(my_half)
    exchange_near(*out)
    out_dst[me] = out_src[me]
    settle(*out)
    arrived = out_dst[...].astype(F32).reshape(slots, ch).astype(BF16)

    def gather_grad(r):
        value = dot(share_t_ref[pl.ds(r * cols, cols)], arrived)
        out_ref[r] = out_ref[r] + value
        value = value.astype(BF16)
        field_ref[1, r] = value
        put_taps(taps_ref, r + 2, value.astype(F32))

    gather_grad(0)
    gather_grad(rows - 1)
    rim_start(1, 0)
    for r in range(1, rows - 1):
        gather_grad(r)
    rim_start(1, 1)

    def put_act(slot, value):
        hidden = hidden_ref[slot]
        value = value * (1.0 - hidden * hidden)
        put_taps(hidden_taps_ref, slot, value.astype(BF16).astype(F32))

    def add_out(r, value):
        out_ref[r] = out_ref[r] + value

    def add_edge(side, value):
        add_out(0 if side == 0 else rows - 1, value)

    outer_inside(adj_second_ref, put_act)
    rim_take(1, 0)
    outer_near(adj_second_ref, put_act)
    inner_near(adj_first_ref, add_out, add_edge)
    rim_take(1, 1)
    outer_far(adj_second_ref, put_act)
    add_out(0, first_tap(hidden_taps_ref, 0, adj_first_ref))
    add_out(rows - 1, last_tap(hidden_taps_ref, rows - 1, adj_first_ref))
    for phase in range(2):
        for depth in range(2):
            rim_sent(phase, depth)


def per_device(
    state,
    background,
    back_precision,
    conv_first,
    bias_first,
    conv_second,
    sounding_tile,
    sounding_cells,
    cell_weights,
    observations,
    live_counts,
    layer_in,
    bias_in,
    layer_out,
    bias_out,
    error_precision,
):
    rows, cols, ch = state.shape
    n = lax.axis_size("dev")
    listed = sounding_tile.shape[0]
    margin = sounding_cells.shape[1]
    slots = 2 * listed
    cap = slots // n
    hid, chan = layer_out.shape
    vmem = pl.BlockSpec(memory_space=pltpu.VMEM)
    hbm = pl.BlockSpec(memory_space=pltpu.HBM)
    dma = pltpu.SemaphoreType.DMA
    operands = tuple(pltpu.with_memory_space_constraint(x, pltpu.HBM) for x in (
        state,
        background,
        back_precision.reshape(1, -1),
        conv_first.reshape(3, 3 * ch, ch),
        bias_first.reshape(1, -1),
        conv_second.reshape(3, 3 * ch, ch),
        sounding_tile.T,
        sounding_cells.T,
        cell_weights.T,
        observations.T,
        layer_in,
        bias_in.reshape(1, -1),
        layer_out.T,
        bias_out,
        error_precision,
    ))
    return pl.pallas_call(
        functools.partial(kernel, n),
        out_shape=jax.ShapeDtypeStruct(state.shape, F32),
        in_specs=[pl.BlockSpec(memory_space=pltpu.SMEM)] + [hbm] * len(operands),
        out_specs=vmem,
        scratch_shapes=[pltpu.VMEM(x.shape, x.dtype) for x in operands]
        + [pltpu.VMEM((12 * ch, 2 * ch), BF16)] * 4
        + [
            pltpu.VMEM((listed, chan), F32),
            pltpu.VMEM((chan, hid), BF16),
            pltpu.VMEM((2, rows, cols, ch), BF16),
            pltpu.VMEM((2, 2, 2, cols, ch), BF16),
            pltpu.VMEM((cols, (rows + 4) * 3 * ch), BF16),
            pltpu.VMEM((rows + 2, cols, ch), F32),
            pltpu.VMEM((cols, (rows + 2) * 3 * ch), BF16),
            pltpu.VMEM((2, cols, ch), F32),
            pltpu.VMEM((2, cols, ch), F32),
            pltpu.VMEM((ch, rows * cols), BF16),
            pltpu.VMEM((2 * margin, listed), F32),
            pltpu.VMEM((listed, slots), BF16),
            pltpu.VMEM((slots, listed), BF16),
            pltpu.VMEM((rows * cols, slots), BF16),
            pltpu.VMEM((listed, ch), BF16),
            pltpu.VMEM((n, 8, LANES), F32),
            pltpu.VMEM((n, 8, LANES), F32),
            pltpu.VMEM((n, cap, ch), BF16),
            pltpu.VMEM((n, cap, ch), BF16),
            pltpu.VMEM((n, cap, ch), BF16),
            pltpu.VMEM((n, cap, ch), BF16),
            dma((len(operands),)),
            dma((2, 2, 2)),
            dma((2, 2, 2)),
            dma((n,)),
            dma((n,)),
            dma((n,)),
            dma((n,)),
            dma((n,)),
            dma((n,)),
        ],
        compiler_params=pltpu.CompilerParams(
            collective_id=0, has_side_effects=True, vmem_limit_bytes=48 * 1024 * 1024
        ),
        name="step",
    )(live_counts, *operands)


def solution(mesh):
    split = P("dev")
    return jax.shard_map(
        per_device,
        mesh=mesh,
        in_specs=(
            split, split, P(), P(), P(), P(), split, split, split, split, split, P(), P(), P(), P(), P(),
        ),
        out_specs=split,
        check_vma=False,
    )
```

```python
import functools

import jax
import jax.numpy as jnp
from jax import lax
from jax.experimental import pallas as pl
from jax.experimental.pallas import tpu as pltpu
from jax.sharding import PartitionSpec as P

F32 = jnp.float32
BF16 = jnp.bfloat16
MESH = pl.DeviceIdType.MESH
LANES = 128


def dot(a, b):
    return jnp.dot(a, b, preferred_element_type=F32)


def dot_nt(a, b):
    return lax.dot_general(a, b, (((1,), (1,)), ((), ())), preferred_element_type=F32)


def kernel(
    n,
    live_ref,
    state_hbm,
    background_hbm,
    back_precision_hbm,
    conv_first_hbm,
    bias_first_hbm,
    conv_second_hbm,
    tile_hbm,
    cells_hbm,
    weights_hbm,
    observations_hbm,
    layer_in_hbm,
    bias_in_hbm,
    layer_out_hbm,
    bias_out_hbm,
    precision_hbm,
    out_ref,
    state_ref,
    background_ref,
    back_precision_ref,
    conv_first_ref,
    bias_first_ref,
    conv_second_ref,
    tile_ref,
    cells_ref,
    weights_ref,
    observations_ref,
    layer_in_ref,
    bias_in_ref,
    layer_out_ref,
    bias_out_ref,
    precision_ref,
    pair_first_ref,
    pair_second_ref,
    adj_first_ref,
    adj_second_ref,
    offset_ref,
    product_ref,
    field_ref,
    halo_ref,
    taps_ref,
    hidden_ref,
    hidden_taps_ref,
    partial_ref,
    edge_ref,
    local_ref,
    share_ref,
    observed_t_ref,
    values_ref,
    place_ref,
    place_t_ref,
    share_t_ref,
    grad_ref,
    req_src,
    req_dst,
    ret_src,
    ret_dst,
    out_src,
    out_dst,
    load_sem,
    halo_send,
    halo_recv,
    req_send,
    req_recv,
    ret_send,
    ret_recv,
    out_send,
    out_recv,
):
    me = lax.axis_index("dev")
    rows, cols, ch = state_ref.shape
    slots, listed = place_t_ref.shape
    cap = slots // n
    per = LANES // cap
    groups = slots // LANES
    half = n // 2
    wide = 3 * ch
    margin = cells_ref.shape[0]
    my_half = lax.div(me, half)
    quarter = n // 4
    my_quarter = lax.div(me, quarter)
    close = 1 - lax.rem(me, 2)

    loads = [
        pltpu.make_async_copy(src, dst, load_sem.at[i])
        for i, (src, dst) in enumerate(
            (
                (tile_hbm, tile_ref),
                (cells_hbm, cells_ref),
                (weights_hbm, weights_ref),
                (state_hbm, state_ref),
                (conv_first_hbm, conv_first_ref),
                (bias_first_hbm, bias_first_ref),
                (precision_hbm, precision_ref),
                (layer_out_hbm, layer_out_ref),
                (conv_second_hbm, conv_second_ref),
                (observations_hbm, observations_ref),
                (bias_out_hbm, bias_out_ref),
                (background_hbm, background_ref),
                (back_precision_hbm, back_precision_ref),
                (layer_in_hbm, layer_in_ref),
                (bias_in_hbm, bias_in_ref),
            )
        )
    ]
    barrier = pltpu.get_barrier_semaphore()

    def far_half(serve):
        def one(j, carry):
            serve((1 - my_half) * half + lax.rem(me + j, half))
            return carry

        lax.fori_loop(0, half, one, 0)

    def near_half(serve):
        def one(j, carry):
            serve(my_half * half + lax.rem(me + j, half))
            return carry

        lax.fori_loop(1, half, one, 0)

    def greet(target):
        pl.semaphore_signal(barrier, inc=1, device_id=(target,), device_id_type=MESH)

    for load in loads[:4]:
        load.start()
    far_half(greet)
    near_half(greet)
    for load in loads[4:]:
        load.start()

    def by_quarters(fill, serve):
        sub = lax.rem(my_quarter, 2)
        for step in range(4):
            which = (my_half if step > 1 else 1 - my_half) * 2 + lax.rem(sub + (step + step // 2) % 2, 2)
            fill(which)

            def one(j, carry):
                serve(which * quarter + lax.rem(me + j, quarter))
                return carry

            lax.fori_loop(1 if step == 3 else 0, quarter, one, 0)

    def post(src, dst, send, recv):
        def one(target):
            pltpu.make_async_remote_copy(
                src_ref=src.at[target],
                dst_ref=dst.at[me],
                send_sem=send,
                recv_sem=recv,
                device_id=(target,),
                device_id_type=MESH,
            ).start()

        return one

    def settle(dst, sem):
        blocks = dst.at[pl.ds(0, n - 1)]
        pltpu.make_async_copy(blocks, blocks, sem).wait()

    def rim(phase, side, depth):
        row = (1 - side) * (rows - 1 - depth) + side * depth
        return pltpu.make_async_remote_copy(
            src_ref=field_ref.at[phase, row],
            dst_ref=halo_ref.at[phase, side, depth],
            send_sem=halo_send.at[phase, side, depth],
            recv_sem=halo_recv.at[phase, side, depth],
            device_id=(lax.rem(me + 1 + side * (n - 2), n),),
            device_id_type=MESH,
        )

    sends = (me < n - 1, me > 0)

    def rim_start(phase, depth):
        for side in range(2):

            @pl.when(sends[side])
            def _():
                rim(phase, side, depth).start()

    def rim_sent(phase, depth):
        for side in range(2):

            @pl.when(sends[side])
            def _():
                rim(phase, side, depth).wait_send()

    def at(start, size):
        return pl.ds(start if isinstance(start, int) else pl.multiple_of(start, LANES), size)

    def put_taps(taps, slot, value):
        taps[:, at(slot * wide, ch)] = pltpu.roll(value, 1, 0).astype(BF16)
        taps[:, at(slot * wide + ch, ch)] = value.astype(BF16)
        taps[:, at(slot * wide + 2 * ch, ch)] = pltpu.roll(value, cols - 1, 0).astype(BF16)

    def rim_take(phase, side, depth):
        slot = 1 - depth + side * (rows + 1 + 2 * depth)

        met = me > 0 if side == 0 else me < n - 1

        @pl.when(met)
        def _():
            rim(phase, side, depth).wait_recv()
            put_taps(taps_ref, slot, halo_ref[phase, side, depth].astype(F32))

        @pl.when(jnp.logical_not(met))
        def _():
            taps_ref[:, pl.ds(slot * wide, wide)] = jnp.zeros((cols, wide), BF16)

    def make_pair(pair_ref, tap):
        zero = jnp.zeros((wide, ch), BF16)
        for a in range(4):
            for o in range(2):
                if 0 <= a - o < 3:
                    for b in range(3):
                        pair_ref[pl.ds(a * wide + b * ch, ch), pl.ds(o * ch, ch)] = tap(a - o, b)
                else:
                    pair_ref[pl.ds(a * wide, wide), pl.ds(o * ch, ch)] = zero

    def plain_of(ref):
        return lambda a, b: ref[a, pl.ds(b * ch, ch)]

    def adjoint_of(ref):
        return lambda a, b: ref[2 - a, pl.ds((2 - b) * ch, ch)].astype(F32).T.astype(BF16)

    def conv_inside(outer, put_outer, inner, put_inner):
        for slot in range(2, rows, 2):
            both = dot(taps_ref[:, pl.ds(slot * wide, 4 * wide)], outer[...])
            put_outer(slot, both[:, :ch])
            put_outer(slot + 1, both[:, ch:])
        for slot in range(2, rows - 2, 2):
            both = dot(hidden_taps_ref[:, pl.ds(slot * wide, 4 * wide)], inner[...])
            put_inner(slot, both[:, :ch])
            put_inner(slot + 1, both[:, ch:])

    def conv_one(side, phase, outer, put_outer, inner, put_inner):
        most = pl.ds((1 - side) * wide, 3 * wide)
        left = pl.ds(side * ch, ch)

        def halves(both):
            return (both[:, ch:], both[:, :ch])[:: 1 - 2 * side]

        rim_take(phase, side, 0)
        done, value = halves(dot(taps_ref[:, pl.ds((1 + side * (rows - 1)) * wide, 3 * wide)], outer[most]))
        partial_ref[...] = value
        put_outer(1 + side * (rows - 1), done)
        done, value = halves(dot(hidden_taps_ref[:, pl.ds((1 + side * (rows - 3)) * wide, 3 * wide)], inner[most]))
        edge_ref[...] = value
        put_inner(1 + side * (rows - 3), done)
        rim_take(phase, side, 1)
        last = pl.ds(side * 3 * wide, wide)
        value = partial_ref[...] + dot(taps_ref[:, pl.ds(side * (rows + 3) * wide, wide)], outer[last, left])
        put_outer(side * (rows + 1), value, (me > 0 if side == 0 else me < n - 1).astype(F32))
        value = edge_ref[...] + dot(hidden_taps_ref[:, pl.ds(side * (rows + 1) * wide, wide)], inner[last, left])
        put_inner(side * (rows - 1), value)

    def conv_side(which, *refs):
        for side in range(2):

            @pl.when(which == side)
            def _():
                conv_one(side, *refs)

    for load in loads[0:3]:
        load.wait()
    tile_row = tile_ref[...].astype(F32)
    tile_col = jnp.broadcast_to(tile_row, (LANES, listed)).T[:, 0:1]
    same = tile_col == tile_row
    from_col = lax.broadcasted_iota(jnp.int32, (listed, listed), 0)
    from_row = lax.broadcasted_iota(jnp.int32, (listed, listed), 1)
    rank_row = jnp.sum(jnp.where(same & (from_col < from_row), 1.0, 0.0), axis=0, keepdims=True)
    slot_row = (tile_row * cap + rank_row).astype(jnp.int32)
    for g in range(groups):
        rowid = lax.broadcasted_iota(jnp.int32, (LANES, listed), 0) + g * LANES
        place_t_ref[pl.ds(g * LANES, LANES)] = jnp.where(rowid == slot_row, 1.0, 0.0).astype(BF16)

    block_of = lax.broadcasted_iota(jnp.int32, (8, LANES), 1) // cap
    row_of = lax.broadcasted_iota(jnp.int32, (8, LANES), 0)
    values_ref[0:margin] = cells_ref[...].astype(F32)
    values_ref[margin : 2 * margin] = weights_ref[...]
    values = values_ref[...]
    part_1 = values.astype(BF16).astype(F32)
    part_2 = (values - part_1).astype(BF16).astype(F32)
    part_3 = values - part_1 - part_2
    parts = jnp.concatenate([part_1, part_2, part_3, jnp.zeros_like(values)], axis=0).astype(BF16)
    held = 2 * margin
    packed = min(held, per)
    on_k = [
        (block_of == k) & (row_of % packed == k) for k in range(packed)
    ]
    for g in range(groups):
        spread = dot_nt(parts, place_t_ref[pl.ds(g * LANES, LANES)])
        spread = spread[0:8] + spread[8:16] + spread[16:24]
        turned = [spread] + [pltpu.roll(spread, d * cap, 1) for d in range(1, per)]
        for i in range(per):
            total = jnp.zeros_like(spread)
            for k in range(packed):
                total = jnp.where(on_k[k], turned[(k + per - i) % per], total)
            reach = 1
            while reach < packed:
                total = total + pltpu.roll(total, held - reach, 0)
                reach = 2 * reach
            for h in range(held // packed):
                req_src[g * per + i, :, pl.ds(h * LANES, LANES)] = total[h * packed : h * packed + 1]
    req_dst[me] = req_src[me]

    loads[3].wait()
    for r in range(rows):
        value = state_ref[r].astype(BF16)
        field_ref[0, r] = value
        put_taps(taps_ref, r + 2, value.astype(F32))

    def put_hidden(slot, value, keep=None):
        value = jnp.tanh(value + bias_first_ref[...]).astype(BF16).astype(F32)
        if keep is not None:
            value = value * keep
        hidden_ref[slot] = value
        put_taps(hidden_taps_ref, slot, value)

    def put_observed(r, value):
        value = state_ref[r] + value
        observed_t_ref[:, at(r * cols, cols)] = value.T.astype(BF16)

    forward = (pair_first_ref, put_hidden, pair_second_ref, put_observed)

    pl.semaphore_wait(barrier, n - 1)
    far_half(post(req_src, req_dst, req_send, req_recv))
    near_half(post(req_src, req_dst, req_send, req_recv))
    rim_start(0, 0)
    rim_start(0, 1)

    loads[4].wait()
    loads[5].wait()
    make_pair(pair_first_ref, plain_of(conv_first_ref))
    loads[8].wait()
    make_pair(pair_second_ref, plain_of(conv_second_ref))

    conv_inside(*forward)
    conv_side(close, 0, *forward)
    settle(req_dst, req_recv)
    for g in range(groups):
        sent = []
        for i in range(per):
            total = jnp.zeros((held, LANES), F32)
            for h in range(held // packed):
                row = jnp.broadcast_to(req_dst[g * per + i, :, pl.ds(h * LANES, LANES)], (held, LANES))
                total = jnp.where(row_of // packed == h, row, total)
            sent.append(total)
        total = jnp.zeros((held, LANES), F32)
        for d in range(per):
            part = jnp.zeros((held, LANES), F32)
            for k in range(packed):
                part = jnp.where(on_k[k], sent[(k + d) % per], part)
            total = total + (pltpu.roll(part, d * cap, 1) if d else part)

        cell = total[0:margin]
        chunk = jnp.floor(cell * (1.0 / LANES))
        local_ref[g] = jnp.concatenate([cell - chunk * LANES, chunk], axis=0)
        share_ref[g] = jnp.concatenate([total[margin:], total[margin:]], axis=0)

    def build_shares(g, carry):
        packs = (LANES // 16, 16, LANES)
        cell = lax.broadcasted_iota(jnp.int32, packs, 0) * 16 + lax.broadcasted_iota(jnp.int32, packs, 1)
        cell = cell.astype(F32).astype(BF16)

        def spread_row(row):
            return jnp.broadcast_to(row, (16, LANES)).astype(BF16)[None]

        local = local_ref[g]
        share = share_ref[g][0:margin]
        hit = [
            jnp.where(cell == spread_row(local[k : k + 1]), 1.0, 0.0).astype(BF16)
            for k in range(margin)
        ]
        for c in range(rows * cols // LANES):
            here = jnp.where(local[margin:] == c, share, 0.0)
            total = hit[0] * spread_row(here[0:1])
            for k in range(1, margin):
                total = total + hit[k] * spread_row(here[k : k + 1])
            share_t_ref[pl.ds(c * LANES, LANES), at(g * LANES, LANES)] = total.reshape(LANES, LANES)
        return carry

    lax.fori_loop(0, groups, build_shares, 0)
    conv_side(1 - close, 0, *forward)

    ret = post(ret_src, ret_dst, ret_send, ret_recv)

    def blend(which):
        base = which * (slots // 2)
        blended = dot(observed_t_ref[...], share_t_ref[:, at(base, slots // 2)]).T
        ret_src[pl.ds(which * half, half)] = blended.reshape(half, cap, ch).astype(BF16)

    blend(1 - my_half)
    far_half(ret)
    blend(my_half)
    near_half(ret)
    ret_dst[me] = ret_src[me]

    rank_col = jnp.sum(jnp.where(same & (from_row < from_col), 1.0, 0.0), axis=1, keepdims=True)
    slot_col = (tile_col * cap + rank_col).astype(jnp.int32)
    for g in range(groups):
        colid = lax.broadcasted_iota(jnp.int32, (listed, LANES), 1) + g * LANES
        place_ref[:, pl.ds(g * LANES, LANES)] = jnp.where(colid == slot_col, 1.0, 0.0).astype(BF16)
    make_pair(adj_second_ref, adjoint_of(conv_second_ref))
    make_pair(adj_first_ref, adjoint_of(conv_first_ref))

    loads[9].wait()
    loads[10].wait()
    bias_out = bias_out_ref[...].reshape(1, -1)
    for s in range(0, listed, LANES):
        offset_ref[pl.ds(s, LANES)] = bias_out - observations_ref[:, pl.ds(s, LANES)].T
    loads[11].wait()
    loads[12].wait()
    for r in range(rows):
        out_ref[r] = back_precision_ref[...] * (state_ref[r] - background_ref[r])
    loads[13].wait()
    loads[14].wait()

    loads[6].wait()
    loads[7].wait()
    chan = precision_ref.shape[0]
    step = 2 * LANES
    for s in range(0, chan, step):
        size = min(step, chan - s)
        wanted_rows = precision_ref[pl.ds(s, size)]
        high = wanted_rows.astype(BF16)
        low = (wanted_rows - high.astype(F32)).astype(BF16)
        product_ref[pl.ds(s, size)] = (
            dot(high, layer_out_ref[...]) + dot(low, layer_out_ref[...])
        ).astype(BF16)

    def flat(ref):
        if cap % 16 == 0:
            return ref[...].reshape(slots, ch)
        return ref[...].astype(F32).reshape(slots, ch).astype(BF16)

    settle(ret_dst, ret_recv)
    returned = flat(ret_dst)
    live = live_ref[0]
    block = listed // 2
    for s in range(0, listed, block):
        span = pl.ds(s, block)
        interpolated = dot(place_ref[span], returned).astype(BF16)
        activated = jnp.tanh(dot(interpolated, layer_in_ref[...]) + bias_in_ref[...]).astype(BF16)
        innovation = dot_nt(activated, layer_out_ref[...]) + offset_ref[span]
        alive = lax.broadcasted_iota(jnp.int32, (block, 1), 0) + s < live
        innovation = jnp.where(alive, innovation, 0.0)
        back_act = dot(innovation.astype(BF16), product_ref[...])
        act_wide = activated.astype(F32)
        pre_grad = (back_act * (1.0 - act_wide * act_wide)).astype(BF16)
        grad_ref[span] = dot_nt(pre_grad, layer_in_ref[...]).astype(BF16)

    out = post(out_src, out_dst, out_send, out_recv)

    def dispatch(which):
        base = which * (slots // 4)
        outgoing = dot(place_t_ref[at(base, slots // 4)], grad_ref[...])
        out_src[pl.ds(which * quarter, quarter)] = outgoing.reshape(quarter, cap, ch).astype(BF16)

    by_quarters(dispatch, out)
    out_dst[me] = out_src[me]
    settle(out_dst, out_recv)
    arrived = flat(out_dst)

    def gather_grad(r):
        value = dot(share_t_ref[pl.ds(r * cols, cols)], arrived)
        out_ref[r] = out_ref[r] + value
        value = value.astype(BF16)
        field_ref[1, r] = value
        put_taps(taps_ref, r + 2, value.astype(F32))

    gather_grad(0)
    gather_grad(rows - 1)
    rim_start(1, 0)
    for r in range(1, rows - 1):
        gather_grad(r)
    rim_start(1, 1)

    def put_act(slot, value, keep=None):
        hidden = hidden_ref[slot]
        value = value * (1.0 - hidden * hidden)
        if keep is not None:
            value = value * keep
        put_taps(hidden_taps_ref, slot, value.astype(BF16).astype(F32))

    def add_out(r, value):
        out_ref[r] = out_ref[r] + value

    backward = (adj_second_ref, put_act, adj_first_ref, add_out)
    conv_inside(*backward)
    conv_side(close, 1, *backward)
    conv_side(1 - close, 1, *backward)
    for phase in range(2):
        for depth in range(2):
            rim_sent(phase, depth)
    settle(req_src, req_send)
    settle(ret_src, ret_send)
    settle(out_src, out_send)


def per_device(
    state,
    background,
    back_precision,
    conv_first,
    bias_first,
    conv_second,
    sounding_tile,
    sounding_cells,
    cell_weights,
    observations,
    live_counts,
    layer_in,
    bias_in,
    layer_out,
    bias_out,
    error_precision,
):
    rows, cols, ch = state.shape
    n = lax.axis_size("dev")
    listed = sounding_tile.shape[0]
    margin = sounding_cells.shape[1]
    slots = 2 * listed
    cap = slots // n
    hid, chan = layer_out.shape
    vmem = pl.BlockSpec(memory_space=pltpu.VMEM)
    hbm = pl.BlockSpec(memory_space=pltpu.HBM)
    dma = pltpu.SemaphoreType.DMA
    operands = tuple(pltpu.with_memory_space_constraint(x, pltpu.HBM) for x in (
        state,
        background,
        back_precision.reshape(1, -1),
        conv_first.reshape(3, 3 * ch, ch),
        bias_first.reshape(1, -1),
        conv_second.reshape(3, 3 * ch, ch),
        sounding_tile.T,
        sounding_cells.T,
        cell_weights.T,
        observations.T,
        layer_in,
        bias_in.reshape(1, -1),
        layer_out.T,
        bias_out,
        error_precision,
    ))
    return pl.pallas_call(
        functools.partial(kernel, n),
        out_shape=jax.ShapeDtypeStruct(state.shape, F32),
        in_specs=[pl.BlockSpec(memory_space=pltpu.SMEM)] + [hbm] * len(operands),
        out_specs=vmem,
        scratch_shapes=[pltpu.VMEM(x.shape, x.dtype) for x in operands]
        + [pltpu.VMEM((12 * ch, 2 * ch), BF16)] * 4
        + [
            pltpu.VMEM((listed, chan), F32),
            pltpu.VMEM((chan, hid), BF16),
            pltpu.VMEM((2, rows, cols, ch), BF16),
            pltpu.VMEM((2, 2, 2, cols, ch), BF16),
            pltpu.VMEM((cols, (rows + 4) * 3 * ch), BF16),
            pltpu.VMEM((rows + 2, cols, ch), F32),
            pltpu.VMEM((cols, (rows + 2) * 3 * ch), BF16),
            pltpu.VMEM((cols, ch), F32),
            pltpu.VMEM((cols, ch), F32),
            pltpu.VMEM((slots // LANES, 2 * margin, LANES), F32),
            pltpu.VMEM((slots // LANES, 2 * margin, LANES), F32),
            pltpu.VMEM((ch, rows * cols), BF16),
            pltpu.VMEM((2 * margin, listed), F32),
            pltpu.VMEM((listed, slots), BF16),
            pltpu.VMEM((slots, listed), BF16),
            pltpu.VMEM((rows * cols, slots), BF16),
            pltpu.VMEM((listed, ch), BF16),
            pltpu.VMEM((n, 1, max(2 * margin * cap, LANES)), F32),
            pltpu.VMEM((n, 1, max(2 * margin * cap, LANES)), F32),
            pltpu.VMEM((n, cap, ch), BF16),
            pltpu.VMEM((n, cap, ch), BF16),
            pltpu.VMEM((n, cap, ch), BF16),
            pltpu.VMEM((n, cap, ch), BF16),
            dma((len(operands),)),
            dma((2, 2, 2)),
            dma((2, 2, 2)),
            dma,
            dma,
            dma,
            dma,
            dma,
            dma,
        ],
        compiler_params=pltpu.CompilerParams(
            collective_id=0, has_side_effects=True, vmem_limit_bytes=48 * 1024 * 1024
        ),
        name="step",
    )(live_counts, *operands)


def solution(mesh):
    split = P("dev")
    return jax.shard_map(
        per_device,
        mesh=mesh,
        in_specs=(
            split, split, P(), P(), P(), P(), split, split, split, split, split, P(), P(), P(), P(), P(),
        ),
        out_specs=split,
        check_vma=False,
    )
```

```python
import functools

import jax
import jax.numpy as jnp
from jax import lax
from jax.experimental import pallas as pl
from jax.experimental.pallas import tpu as pltpu
from jax.sharding import PartitionSpec as P

F32 = jnp.float32
BF16 = jnp.bfloat16
MESH = pl.DeviceIdType.MESH
LANES = 128


def dot(a, b):
    return jnp.dot(a, b, preferred_element_type=F32)


def dot_nt(a, b):
    return lax.dot_general(a, b, (((1,), (1,)), ((), ())), preferred_element_type=F32)


def kernel(
    n,
    live_ref,
    state_hbm,
    background_hbm,
    back_precision_hbm,
    conv_first_hbm,
    bias_first_hbm,
    conv_second_hbm,
    tile_hbm,
    cells_hbm,
    weights_hbm,
    observations_hbm,
    layer_in_hbm,
    bias_in_hbm,
    layer_out_hbm,
    bias_out_hbm,
    precision_hbm,
    out_ref,
    state_ref,
    background_ref,
    back_precision_ref,
    conv_first_ref,
    bias_first_ref,
    conv_second_ref,
    tile_ref,
    cells_ref,
    weights_ref,
    observations_ref,
    layer_in_ref,
    bias_in_ref,
    layer_out_ref,
    bias_out_ref,
    precision_ref,
    pair_first_ref,
    pair_second_ref,
    adj_first_ref,
    adj_second_ref,
    offset_ref,
    product_ref,
    field_ref,
    halo_ref,
    taps_ref,
    hidden_ref,
    hidden_taps_ref,
    partial_ref,
    edge_ref,
    local_ref,
    share_ref,
    near_ref,
    gathered_ref,
    observed_t_ref,
    values_ref,
    place_ref,
    place_t_ref,
    share_t_ref,
    grad_ref,
    req_src,
    req_dst,
    ret_src,
    ret_dst,
    out_src,
    out_dst,
    load_sem,
    halo_send,
    halo_recv,
    req_send,
    req_recv,
    ret_send,
    ret_recv,
    out_send,
    out_recv,
):
    me = lax.axis_index("dev")
    rows, cols, ch = state_ref.shape
    slots, listed = place_t_ref.shape
    cap = slots // n
    per = LANES // cap
    groups = slots // LANES
    half = n // 2
    wide = 3 * ch
    margin = cells_ref.shape[0]
    my_half = lax.div(me, half)
    quarter = n // 4
    my_quarter = lax.div(me, quarter)
    close = 1 - lax.rem(me, 2)

    loads = [
        pltpu.make_async_copy(src, dst, load_sem.at[i])
        for i, (src, dst) in enumerate(
            (
                (tile_hbm, tile_ref),
                (cells_hbm, cells_ref),
                (weights_hbm, weights_ref),
                (state_hbm, state_ref),
                (conv_first_hbm, conv_first_ref),
                (bias_first_hbm, bias_first_ref),
                (precision_hbm, precision_ref),
                (layer_out_hbm, layer_out_ref),
                (conv_second_hbm, conv_second_ref),
                (observations_hbm, observations_ref),
                (bias_out_hbm, bias_out_ref),
                (background_hbm, background_ref),
                (back_precision_hbm, back_precision_ref),
                (layer_in_hbm, layer_in_ref),
                (bias_in_hbm, bias_in_ref),
            )
        )
    ]
    barrier = pltpu.get_barrier_semaphore()

    def far_half(serve):
        def one(j, carry):
            serve((1 - my_half) * half + lax.rem(me + j, half))
            return carry

        lax.fori_loop(0, half, one, 0)

    def near_half(serve):
        def one(j, carry):
            serve(my_half * half + lax.rem(me + j, half))
            return carry

        lax.fori_loop(1, half, one, 0)

    def greet(target):
        pl.semaphore_signal(barrier, inc=1, device_id=(target,), device_id_type=MESH)

    for load in loads[:4]:
        load.start()
    far_half(greet)
    near_half(greet)
    for load in loads[4:]:
        load.start()

    outer = ((my_quarter == 0) | (my_quarter == 3)).astype(jnp.int32)

    def by_quarters(fill, serve):
        sub = lax.rem(my_quarter, 2)
        far_a = (1 - my_half) * 2 + sub
        far_b = (1 - my_half) * 2 + 1 - sub
        beside = my_half * 2 + 1 - sub
        first = ((far_a, far_a), (far_b, beside), (beside, far_b), (my_quarter, my_quarter))
        is_near = ((0, 0), (0, 1), (1, 0), (1, 1))
        for step in range(4):
            which = first[step][0] * (1 - outer) + first[step][1] * outer
            near = is_near[step][0] * (1 - outer) + is_near[step][1] * outer
            fill(which)

            def one(j, carry):
                serve(which * quarter + lax.rem(me + j, quarter), near)
                return carry

            lax.fori_loop(1 if step == 3 else 0, quarter, one, 0)

    def by_halves(fill, serve):
        for step in range(2):
            near = step
            which = my_half if near else 1 - my_half
            fill(which)

            def one(j, carry):
                serve(which * half + lax.rem(me + j + near, half), near)
                return carry

            lax.fori_loop(0, half - near, one, 0)

    def post(src, dst, send, recv):
        def one(target, near=None):
            pltpu.make_async_remote_copy(
                src_ref=src.at[target],
                dst_ref=dst.at[me],
                send_sem=send,
                recv_sem=recv if near is None else recv.at[near],
                device_id=(target,),
                device_id_type=MESH,
            ).start()

        return one

    def settle(dst, sem, count):
        blocks = dst.at[pl.ds(0, count)]
        pltpu.make_async_copy(blocks, blocks, sem).wait()

    def rim(phase, side, depth):
        row = (1 - side) * (rows - 1 - depth) + side * depth
        return pltpu.make_async_remote_copy(
            src_ref=field_ref.at[phase, row],
            dst_ref=halo_ref.at[phase, side, depth],
            send_sem=halo_send.at[phase, side, depth],
            recv_sem=halo_recv.at[phase, side, depth],
            device_id=(lax.rem(me + 1 + side * (n - 2), n),),
            device_id_type=MESH,
        )

    def rim_start(phase, side, depth):
        @pl.when(((side == 0) & (me < n - 1)) | ((side == 1) & (me > 0)))
        def _():
            rim(phase, side, depth).start()

    def rim_sent(phase, depth):
        for side in range(2):

            @pl.when(me < n - 1 if side == 0 else me > 0)
            def _():
                rim(phase, side, depth).wait_send()

    def at(start, size):
        return pl.ds(start if isinstance(start, int) else pl.multiple_of(start, LANES), size)

    def put_taps(taps, slot, value):
        taps[:, at(slot * wide, ch)] = pltpu.roll(value, 1, 0).astype(BF16)
        taps[:, at(slot * wide + ch, ch)] = value.astype(BF16)
        taps[:, at(slot * wide + 2 * ch, ch)] = pltpu.roll(value, cols - 1, 0).astype(BF16)

    def rim_take(phase, side, depth):
        slot = 1 - depth + side * (rows + 1 + 2 * depth)

        met = me > 0 if side == 0 else me < n - 1

        @pl.when(met)
        def _():
            rim(phase, side, depth).wait_recv()
            put_taps(taps_ref, slot, halo_ref[phase, side, depth].astype(F32))

        @pl.when(jnp.logical_not(met))
        def _():
            taps_ref[:, pl.ds(slot * wide, wide)] = jnp.zeros((cols, wide), BF16)

    def make_pair(pair_ref, tap):
        zero = jnp.zeros((wide, ch), BF16)
        for a in range(4):
            for o in range(2):
                if 0 <= a - o < 3:
                    for b in range(3):
                        pair_ref[pl.ds(a * wide + b * ch, ch), pl.ds(o * ch, ch)] = tap(a - o, b)
                else:
                    pair_ref[pl.ds(a * wide, wide), pl.ds(o * ch, ch)] = zero

    def plain_of(ref):
        return lambda a, b: ref[a, pl.ds(b * ch, ch)]

    def adjoint_of(ref):
        return lambda a, b: ref[2 - a, pl.ds((2 - b) * ch, ch)].astype(F32).T.astype(BF16)

    def conv_inside(outer, put_outer, inner, put_inner):
        for slot in range(2, rows, 2):
            both = dot(taps_ref[:, pl.ds(slot * wide, 4 * wide)], outer[...])
            put_outer(slot, both[:, :ch])
            put_outer(slot + 1, both[:, ch:])
        for slot in range(2, rows - 2, 2):
            both = dot(hidden_taps_ref[:, pl.ds(slot * wide, 4 * wide)], inner[...])
            put_inner(slot, both[:, :ch])
            put_inner(slot + 1, both[:, ch:])

    def conv_one(side, phase, outer, put_outer, inner, put_inner):
        most = pl.ds((1 - side) * wide, 3 * wide)
        left = pl.ds(side * ch, ch)

        def halves(both):
            return (both[:, ch:], both[:, :ch])[:: 1 - 2 * side]

        rim_take(phase, side, 0)
        done, value = halves(dot(taps_ref[:, pl.ds((1 + side * (rows - 1)) * wide, 3 * wide)], outer[most]))
        partial_ref[...] = value
        put_outer(1 + side * (rows - 1), done)
        done, value = halves(dot(hidden_taps_ref[:, pl.ds((1 + side * (rows - 3)) * wide, 3 * wide)], inner[most]))
        edge_ref[...] = value
        put_inner(1 + side * (rows - 3), done)
        rim_take(phase, side, 1)
        last = pl.ds(side * 3 * wide, wide)
        value = partial_ref[...] + dot(taps_ref[:, pl.ds(side * (rows + 3) * wide, wide)], outer[last, left])
        put_outer(side * (rows + 1), value, (me > 0 if side == 0 else me < n - 1).astype(F32))
        value = edge_ref[...] + dot(hidden_taps_ref[:, pl.ds(side * (rows + 1) * wide, wide)], inner[last, left])
        put_inner(side * (rows - 1), value)

    def conv_side(which, *refs):
        for side in range(2):

            @pl.when(which == side)
            def _():
                conv_one(side, *refs)

    for load in loads[0:3]:
        load.wait()
    tile_row = tile_ref[...].astype(F32)
    tile_col = jnp.broadcast_to(tile_row, (LANES, listed)).T[:, 0:1]
    same = tile_col == tile_row
    from_col = lax.broadcasted_iota(jnp.int32, (listed, listed), 0)
    from_row = lax.broadcasted_iota(jnp.int32, (listed, listed), 1)
    rank_row = jnp.sum(jnp.where(same & (from_col < from_row), 1.0, 0.0), axis=0, keepdims=True)
    slot_row = (tile_row * cap + rank_row).astype(jnp.int32)
    for g in range(groups):
        rowid = lax.broadcasted_iota(jnp.int32, (LANES, listed), 0) + g * LANES
        place_t_ref[pl.ds(g * LANES, LANES)] = jnp.where(rowid == slot_row, 1.0, 0.0).astype(BF16)

    block_of = lax.broadcasted_iota(jnp.int32, (8, LANES), 1) // cap
    row_of = lax.broadcasted_iota(jnp.int32, (8, LANES), 0)
    values_ref[0:margin] = cells_ref[...].astype(F32)
    values_ref[margin : 2 * margin] = weights_ref[...]
    values = values_ref[...]
    part_1 = values.astype(BF16).astype(F32)
    part_2 = (values - part_1).astype(BF16).astype(F32)
    part_3 = values - part_1 - part_2
    parts = jnp.concatenate([part_1, part_2, part_3, jnp.zeros_like(values)], axis=0).astype(BF16)
    held = 2 * margin
    packed = min(held, per)
    on_k = [
        (block_of == k) & (row_of % packed == k) for k in range(packed)
    ]
    for g in range(groups):
        spread = dot_nt(parts, place_t_ref[pl.ds(g * LANES, LANES)])
        spread = spread[0:8] + spread[8:16] + spread[16:24]
        turned = [spread] + [pltpu.roll(spread, d * cap, 1) for d in range(1, per)]
        for i in range(per):
            total = jnp.zeros_like(spread)
            for k in range(packed):
                total = jnp.where(on_k[k], turned[(k + per - i) % per], total)
            reach = 1
            while reach < packed:
                total = total + pltpu.roll(total, held - reach, 0)
                reach = 2 * reach
            for h in range(held // packed):
                req_src[g * per + i, :, pl.ds(h * LANES, LANES)] = total[h * packed : h * packed + 1]
    req_dst[me] = req_src[me]

    loads[3].wait()
    for r in range(rows):
        value = state_ref[r].astype(BF16)
        field_ref[0, r] = value
        put_taps(taps_ref, r + 2, value.astype(F32))

    def put_hidden(slot, value, keep=None):
        value = jnp.tanh(value + bias_first_ref[...]).astype(BF16).astype(F32)
        if keep is not None:
            value = value * keep
        hidden_ref[slot] = value
        put_taps(hidden_taps_ref, slot, value)

    def put_observed(r, value):
        value = state_ref[r] + value
        observed_t_ref[:, at(r * cols, cols)] = value.T.astype(BF16)

    forward = (pair_first_ref, put_hidden, pair_second_ref, put_observed)

    pl.semaphore_wait(barrier, n - 1)
    far_half(post(req_src, req_dst, req_send, req_recv))
    near_half(post(req_src, req_dst, req_send, req_recv))
    for side in (close, 1 - close):
        for depth in range(2):
            rim_start(0, side, depth)

    loads[4].wait()
    loads[5].wait()
    make_pair(pair_first_ref, plain_of(conv_first_ref))
    loads[8].wait()
    make_pair(pair_second_ref, plain_of(conv_second_ref))

    conv_inside(*forward)
    conv_side(close, 0, *forward)
    settle(req_dst, req_recv, n - 1)
    for g in range(groups):
        sent = []
        for i in range(per):
            total = jnp.zeros((held, LANES), F32)
            for h in range(held // packed):
                row = jnp.broadcast_to(req_dst[g * per + i, :, pl.ds(h * LANES, LANES)], (held, LANES))
                total = jnp.where(row_of // packed == h, row, total)
            sent.append(total)
        total = jnp.zeros((held, LANES), F32)
        for d in range(per):
            part = jnp.zeros((held, LANES), F32)
            for k in range(packed):
                part = jnp.where(on_k[k], sent[(k + d) % per], part)
            total = total + (pltpu.roll(part, d * cap, 1) if d else part)

        cell = total[0:margin]
        chunk = jnp.floor(cell * (1.0 / LANES))
        local_ref[g] = jnp.concatenate([cell - chunk * LANES, chunk], axis=0)
        share_ref[g] = jnp.concatenate([total[margin:], total[margin:]], axis=0)

    def build_shares(g, carry):
        packs = (LANES // 16, 16, LANES)
        cell = lax.broadcasted_iota(jnp.int32, packs, 0) * 16 + lax.broadcasted_iota(jnp.int32, packs, 1)
        cell = cell.astype(F32).astype(BF16)

        def spread_row(row):
            return jnp.broadcast_to(row, (16, LANES)).astype(BF16)

        local = local_ref[g]
        share = share_ref[g]
        chunk = [spread_row(local[margin + k : margin + k + 1]) for k in range(margin)]
        weight = [spread_row(share[k : k + 1]) for k in range(margin)]
        hit = [
            jnp.where(cell == spread_row(local[k : k + 1])[None], 1.0, 0.0).astype(BF16)
            for k in range(margin)
        ]
        for c in range(rows * cols // LANES):
            total = None
            for k in range(margin):
                here = jnp.where(chunk[k] == c, weight[k], jnp.zeros_like(weight[k]))
                term = hit[k] * here[None]
                total = term if total is None else total + term
            share_t_ref[pl.ds(c * LANES, LANES), at(g * LANES, LANES)] = total.reshape(LANES, LANES)
        return carry

    lax.fori_loop(0, groups, build_shares, 0)
    conv_side(1 - close, 0, *forward)


    def blend(which):
        base = which * (slots // 2)
        blended = dot(observed_t_ref[...], share_t_ref[:, at(base, slots // 2)]).T
        ret_src[pl.ds(which * half, half)] = blended.reshape(half, cap, ch).astype(BF16)

    by_halves(blend, post(ret_src, ret_dst, ret_send, ret_recv))
    ret_dst[me] = ret_src[me]

    rank_col = jnp.sum(jnp.where(same & (from_row < from_col), 1.0, 0.0), axis=1, keepdims=True)
    slot_col = (tile_col * cap + rank_col).astype(jnp.int32)
    for g in range(groups):
        colid = lax.broadcasted_iota(jnp.int32, (listed, LANES), 1) + g * LANES
        place_ref[:, pl.ds(g * LANES, LANES)] = jnp.where(colid == slot_col, 1.0, 0.0).astype(BF16)
    make_pair(adj_second_ref, adjoint_of(conv_second_ref))
    make_pair(adj_first_ref, adjoint_of(conv_first_ref))

    loads[9].wait()
    loads[10].wait()
    bias_out = bias_out_ref[...].reshape(1, -1)
    for s in range(0, listed, LANES):
        offset_ref[pl.ds(s, LANES)] = bias_out - observations_ref[:, pl.ds(s, LANES)].T
    loads[11].wait()
    loads[12].wait()
    for r in range(rows):
        out_ref[r] = back_precision_ref[...] * (state_ref[r] - background_ref[r])
    loads[13].wait()
    loads[14].wait()

    loads[6].wait()
    loads[7].wait()
    chan = precision_ref.shape[0]
    step = 2 * LANES
    for s in range(0, chan, step):
        size = min(step, chan - s)
        wanted_rows = precision_ref[pl.ds(s, size)]
        high = wanted_rows.astype(BF16)
        low = (wanted_rows - high.astype(F32)).astype(BF16)
        product_ref[pl.ds(s, size)] = (
            dot(high, layer_out_ref[...]) + dot(low, layer_out_ref[...])
        ).astype(BF16)

    def flat(ref, which):
        blocks = ref[pl.ds(which * half, half)]
        if cap % 16 == 0:
            return blocks.reshape(half * cap, ch)
        return blocks.astype(F32).reshape(half * cap, ch).astype(BF16)

    near_lanes = at(my_half * (slots // 2), slots // 2)
    far_lanes = at((1 - my_half) * (slots // 2), slots // 2)

    settle(ret_dst, ret_recv.at[1], half - 1)
    near_ref[...] = dot(place_ref[:, near_lanes], flat(ret_dst, my_half))
    settle(ret_dst, ret_recv.at[0], half)
    returned = flat(ret_dst, 1 - my_half)
    live = live_ref[0]
    block = listed // 2
    for s in range(0, listed, block):
        span = pl.ds(s, block)
        interpolated = (near_ref[span] + dot(place_ref[span, far_lanes], returned)).astype(BF16)
        activated = jnp.tanh(dot(interpolated, layer_in_ref[...]) + bias_in_ref[...]).astype(BF16)
        innovation = dot_nt(activated, layer_out_ref[...]) + offset_ref[span]
        alive = lax.broadcasted_iota(jnp.int32, (block, 1), 0) + s < live
        innovation = jnp.where(alive, innovation, 0.0)
        back_act = dot(innovation.astype(BF16), product_ref[...])
        act_wide = activated.astype(F32)
        pre_grad = (back_act * (1.0 - act_wide * act_wide)).astype(BF16)
        grad_ref[span] = dot_nt(pre_grad, layer_in_ref[...]).astype(BF16)


    def dispatch(which):
        base = which * (slots // 4)
        outgoing = dot(place_t_ref[at(base, slots // 4)], grad_ref[...])
        out_src[pl.ds(which * quarter, quarter)] = outgoing.reshape(quarter, cap, ch).astype(BF16)

    by_quarters(dispatch, post(out_src, out_dst, out_send, out_recv))
    out_dst[me] = out_src[me]
    settle(out_dst, out_recv.at[1], half - 1)
    arrived = flat(out_dst, my_half)
    for r in range(rows):
        gathered_ref[r] = dot(share_t_ref[pl.ds(r * cols, cols), near_lanes], arrived)
    settle(out_dst, out_recv.at[0], half)

    def gather_grad(r):
        arrived = flat(out_dst, 1 - my_half)
        value = gathered_ref[r] + dot(share_t_ref[at(r * cols, cols), far_lanes], arrived)
        field_ref[1, r] = value.astype(BF16)
        out_ref[r] = out_ref[r] + value

    for side in (close, 1 - close):
        for depth in range(2):
            gather_grad((1 - side) * (rows - 1 - depth) + side * depth)
            rim_start(1, side, depth)
    for r in range(2, rows - 2):
        gather_grad(r)
    for r in range(rows):
        put_taps(taps_ref, r + 2, field_ref[1, r].astype(F32))

    def put_act(slot, value, keep=None):
        hidden = hidden_ref[slot]
        value = value * (1.0 - hidden * hidden)
        if keep is not None:
            value = value * keep
        put_taps(hidden_taps_ref, slot, value.astype(BF16).astype(F32))

    def add_out(r, value):
        out_ref[r] = out_ref[r] + value

    backward = (adj_second_ref, put_act, adj_first_ref, add_out)
    conv_inside(*backward)
    conv_side(close, 1, *backward)
    conv_side(1 - close, 1, *backward)
    for phase in range(2):
        for depth in range(2):
            rim_sent(phase, depth)
    settle(req_src, req_send, n - 1)
    settle(ret_src, ret_send, n - 1)
    settle(out_src, out_send, n - 1)


def per_device(
    state,
    background,
    back_precision,
    conv_first,
    bias_first,
    conv_second,
    sounding_tile,
    sounding_cells,
    cell_weights,
    observations,
    live_counts,
    layer_in,
    bias_in,
    layer_out,
    bias_out,
    error_precision,
):
    rows, cols, ch = state.shape
    n = lax.axis_size("dev")
    listed = sounding_tile.shape[0]
    margin = sounding_cells.shape[1]
    slots = 2 * listed
    cap = slots // n
    hid, chan = layer_out.shape
    vmem = pl.BlockSpec(memory_space=pltpu.VMEM)
    hbm = pl.BlockSpec(memory_space=pltpu.HBM)
    dma = pltpu.SemaphoreType.DMA
    operands = tuple(pltpu.with_memory_space_constraint(x, pltpu.HBM) for x in (
        state,
        background,
        back_precision.reshape(1, -1),
        conv_first.reshape(3, 3 * ch, ch),
        bias_first.reshape(1, -1),
        conv_second.reshape(3, 3 * ch, ch),
        sounding_tile.T,
        sounding_cells.T,
        cell_weights.T,
        observations.T,
        layer_in,
        bias_in.reshape(1, -1),
        layer_out.T,
        bias_out,
        error_precision,
    ))
    return pl.pallas_call(
        functools.partial(kernel, n),
        out_shape=jax.ShapeDtypeStruct(state.shape, F32),
        in_specs=[pl.BlockSpec(memory_space=pltpu.SMEM)] + [hbm] * len(operands),
        out_specs=vmem,
        scratch_shapes=[pltpu.VMEM(x.shape, x.dtype) for x in operands]
        + [pltpu.VMEM((12 * ch, 2 * ch), BF16)] * 4
        + [
            pltpu.VMEM((listed, chan), F32),
            pltpu.VMEM((chan, hid), BF16),
            pltpu.VMEM((2, rows, cols, ch), BF16),
            pltpu.VMEM((2, 2, 2, cols, ch), BF16),
            pltpu.VMEM((cols, (rows + 4) * 3 * ch), BF16),
            pltpu.VMEM((rows + 2, cols, ch), F32),
            pltpu.VMEM((cols, (rows + 2) * 3 * ch), BF16),
            pltpu.VMEM((cols, ch), F32),
            pltpu.VMEM((cols, ch), F32),
            pltpu.VMEM((slots // LANES, 2 * margin, LANES), F32),
            pltpu.VMEM((slots // LANES, 2 * margin, LANES), F32),
            pltpu.VMEM((listed, ch), F32),
            pltpu.VMEM(state.shape, F32),
            pltpu.VMEM((ch, rows * cols), BF16),
            pltpu.VMEM((2 * margin, listed), F32),
            pltpu.VMEM((listed, slots), BF16),
            pltpu.VMEM((slots, listed), BF16),
            pltpu.VMEM((rows * cols, slots), BF16),
            pltpu.VMEM((listed, ch), BF16),
            pltpu.VMEM((n, 1, max(2 * margin * cap, LANES)), F32),
            pltpu.VMEM((n, 1, max(2 * margin * cap, LANES)), F32),
            pltpu.VMEM((n, cap, ch), BF16),
            pltpu.VMEM((n, cap, ch), BF16),
            pltpu.VMEM((n, cap, ch), BF16),
            pltpu.VMEM((n, cap, ch), BF16),
            dma((len(operands),)),
            dma((2, 2, 2)),
            dma((2, 2, 2)),
            dma,
            dma,
            dma,
            dma((2,)),
            dma,
            dma((2,)),
        ],
        compiler_params=pltpu.CompilerParams(
            collective_id=0, has_side_effects=True, vmem_limit_bytes=48 * 1024 * 1024
        ),
        name="step",
    )(live_counts, *operands)


def solution(mesh):
    split = P("dev")
    return jax.shard_map(
        per_device,
        mesh=mesh,
        in_specs=(
            split, split, P(), P(), P(), P(), split, split, split, split, split, P(), P(), P(), P(), P(),
        ),
        out_specs=split,
        check_vma=False,
    )
```
